32 devices in a mesh: mp: 4 (over z), latent: 8 (over y, x, core).
Axes of the slice: x: 2, y: 2, z: 4, core: 2. Of those that a mesh axis runs over, the one named last changes fastest.
Arguments:
- clean_stream: bfloat16 [128, 4608], P('latent', 'mp'), may hold values from -64 to 64
- patch_stream: bfloat16 [128, 4608], P('latent', 'mp'), may hold values from -64 to 64
- output_grad: bfloat16 [128, 4608], P('latent', 'mp'), may hold values from -1.5 to 1.5
- input_gain: float32 [4608], P('mp'), may hold values from 0.25 to 1.75
- gate_weight: bfloat16 [4608, 18432], P('mp', 'latent'), may hold values from -0.09375 to 0.09375
- up_weight: bfloat16 [4608, 18432], P('mp', 'latent'), may hold values from -0.09375 to 0.09375
- down_weight: bfloat16 [18432, 4608], P('latent', 'mp'), may hold values from -0.125 to 0.125
- output_gain: float32 [4608], P('mp'), may hold values from 0.25 to 1.75
- encoder_weight: bfloat16 [4608, 8192], P('mp', 'latent'), may hold values from -0.09375 to 0.09375
- encoder_bias: float32 [8192], P('latent'), may hold values from -1 to 0.3
- decoder_weight: bfloat16 [8192, 4608], P('latent', 'mp'), may hold values from -0.09375 to 0.09375
- decoder_bias: float32 [4608], P('mp'), may hold values from -3 to 3
- patch_positions: int32 [1, 8], replicated, may hold values from 0 to 127
Outputs:
- layer_output: bfloat16 [128, 4608], P('latent', 'mp')
- latent_effects: float32 [1, 8192], P(None, 'latent')
- position_effects: float32 [1, 8, 8192], P(None, None, 'latent')
The draws below stay inside these ranges and needn't reach their ends.
All inputs are finite; a program needn't handle non-finite values.
Results may differ from the reference program's by a relative error of at most 0.017.
Values may be sent and summed in bfloat16 or wider, within the bound.
No kernel may reach another device: no remote copies, remote signals or barrier semaphores. Data moves between devices by JAX's collectives and lax.ppermute only.
A program may use at most 64 MiB of HBM per device.

```python
import math
import jax
import jax.numpy as jnp
from jax import lax

D = 4608
FF = 18432
LAT_DEV = 256
SEQS = 1
SEQ = 128
P_SIZE = 8
TOK = 128
LATENTS = 8192
N_MP = 4
N_LATENT = 8


def column_scales(key, salt):
    spread = jax.random.uniform(jax.random.fold_in(key, salt), (D,), jnp.float32)
    trend = jnp.arange(D, dtype=jnp.float32) / D - 0.5
    return jnp.exp(math.log(10.0) * (spread - 0.5) + math.log(3.0) * trend)


def stream_draw(key, which):
    count = SEQS * SEQ
    columns = column_scales(key, 101)
    row_spread = jax.random.uniform(jax.random.fold_in(key, 200 + which), (count, 1), jnp.float32)
    row_scales = jnp.exp(math.log(10.0) * (row_spread - 0.5))
    noise_key = jax.random.fold_in(key, 300 + which)
    noise = jnp.clip(jax.random.normal(noise_key, (count, D), jnp.float32), -4.0, 4.0)
    return jnp.clip(noise * row_scales * columns, -64.0, 64.0).astype(jnp.bfloat16)


def draw_clean_stream(key, part):
    return stream_draw(key, 1)


def draw_patch_stream(key, part):
    return stream_draw(key, 2)


def draw_down_weight(key, part):
    columns = column_scales(key, 501)
    noise_key = jax.random.fold_in(key, 502)
    noise = jnp.clip(jax.random.normal(noise_key, (FF, D), jnp.float32), -4.0, 4.0)
    return jnp.clip(noise * columns / math.sqrt(FF), -0.125, 0.125).astype(jnp.bfloat16)


def with_ends(result, own_key, smallest, largest):
    dims = result.shape
    index_at = [jax.random.randint(jax.random.fold_in(own_key, axis), (), 0, dims[axis]) for axis in range(len(dims))]
    result = result.at[tuple(index_at)].set(smallest)
    longest = dims.index(max(dims))
    index_at[longest] = (index_at[longest] + 1) % dims[longest]
    return result.at[tuple(index_at)].set(largest)


def steps_of(rng, shape, shards, least, high):
    loudness = 1.0
    for axis_at, parts in shards:
        draws = jax.random.uniform(jax.random.fold_in(jax.random.fold_in(rng, 6), axis_at), (parts,), jnp.float32, least / len(shards), high / len(shards))
        loudness = loudness * jnp.repeat(jnp.exp(draws), shape[axis_at] // parts).reshape((-1,) + (1,) * (len(shape) - 1 - axis_at))
    return loudness


def centred(stream_key, dims, width, reach, split=(), kind=jnp.bfloat16):
    entries = jax.random.normal(stream_key, dims, jnp.float32) * width
    if len(split) > 0:
        entries = steps_of(stream_key, dims, split, -0.22, 0.18) * entries
    return jnp.clip(entries, min=-reach, max=reach).astype(kind)


def setup_inputs(seed: int = 0) -> dict:
    seeds = jax.random.split(jax.random.key(seed), 14)
    clean_stream = draw_clean_stream(jax.random.fold_in(seeds[13], 71), 0)
    patch_stream = draw_patch_stream(jax.random.fold_in(seeds[13], 71), 0)
    output_grad = centred(seeds[2], (TOK, D), 0.25, 1.5, ((0, 8), (1, 4)))
    input_gain = jnp.clip(1.0 + 0.15 * jax.random.normal(seeds[3], (D,), jnp.float32), 0.25, 1.75)
    gate_weight = centred(seeds[4], (D, FF), D ** -0.5, 0.09375, ((0, 4), (1, 8)))
    up_weight = centred(seeds[5], (D, FF), D ** -0.5, 0.09375, ((0, 4), (1, 8)))
    down_weight = draw_down_weight(jax.random.fold_in(seeds[13], 71), 0)
    output_gain = jnp.clip(1.0 + 0.15 * jax.random.normal(seeds[7], (D,), jnp.float32), 0.25, 1.75)
    encoder_weight = centred(seeds[8], (D, LATENTS), D ** -0.5, 0.09375, ((0, 4), (1, 8)))
    encoder_bias = jnp.clip(-1.0 + 1.3 * jax.random.uniform(seeds[9], (LATENTS,), jnp.float32) ** steps_of(seeds[9], (LATENTS,), ((0, 8),), -0.2, 0.2), -1.0, 0.3)
    decoder_weight = centred(seeds[10], (LATENTS, D), D ** -0.5, 0.09375, ((0, 8), (1, 4)))
    decoder_bias = centred(seeds[11], (D,), 0.5, 3.0, ((0, 4),), jnp.float32)
    patch_positions = with_ends(jax.random.randint(seeds[12], (SEQS, P_SIZE), 0, SEQ), jax.random.fold_in(seeds[12], 1), 0, SEQ - 1).astype(jnp.int32)
    return {"clean_stream": clean_stream, "patch_stream": patch_stream, "output_grad": output_grad, "input_gain": input_gain, "gate_weight": gate_weight, "up_weight": up_weight, "down_weight": down_weight, "output_gain": output_gain, "encoder_weight": encoder_weight, "encoder_bias": encoder_bias, "decoder_weight": decoder_weight, "decoder_bias": decoder_bias, "patch_positions": patch_positions}


epsilon = 1e-06
tanh_scale = 0.7978845608028654
cubic_term = 0.044715

def gelu_parts(gate_sum):
    inner = tanh_scale * (gate_sum + cubic_term * gate_sum * gate_sum * gate_sum)
    tangent = jnp.tanh(inner)
    gelu_value = 0.5 * gate_sum * (1.0 + tangent)
    gelu_slope = 0.5 * (1.0 + tangent) + 0.5 * gate_sum * (1.0 - tangent * tangent) * tanh_scale * (1.0 + 3.0 * cubic_term * gate_sum * gate_sum)
    return (gelu_value, gelu_slope)

def dot_transposed(left, right):
    return lax.dot_general(left, right, (((1,), (1,)), ((), ())), preferred_element_type=jnp.float32)

def reference(clean_stream, patch_stream, output_grad, input_gain, gate_weight, up_weight, down_weight, output_gain, encoder_weight, encoder_bias, decoder_weight, decoder_bias, patch_positions):
    clean_rows = clean_stream.astype(jnp.float32)
    in_scale = lax.rsqrt(lax.optimization_barrier(jnp.mean(clean_rows * clean_rows, axis=1, keepdims=True)) + epsilon)
    normed = (clean_rows * in_scale * input_gain).astype(jnp.bfloat16)
    gate_sum = jnp.dot(normed, gate_weight, preferred_element_type=jnp.float32)
    up_sum = jnp.dot(normed, up_weight, preferred_element_type=jnp.float32)
    gelu_value, gelu_slope = gelu_parts(gate_sum)
    hidden = (gelu_value * up_sum).astype(jnp.bfloat16)
    mlp_out = jnp.dot(hidden, down_weight, preferred_element_type=jnp.float32)
    out_scale = lax.rsqrt(lax.optimization_barrier(jnp.mean(mlp_out * mlp_out, axis=1, keepdims=True)) + epsilon)
    layer_output = (clean_rows + mlp_out * out_scale * output_gain).astype(jnp.bfloat16)
    grad_rows = output_grad.astype(jnp.float32)
    weighted_out = output_gain * grad_rows
    cross_out = lax.optimization_barrier(jnp.mean(mlp_out * weighted_out, axis=1, keepdims=True))
    mlp_grad = (out_scale * weighted_out - mlp_out * out_scale * out_scale * out_scale * cross_out).astype(jnp.bfloat16)
    hidden_grad = dot_transposed(mlp_grad, down_weight)
    gate_grad = (hidden_grad * up_sum * gelu_slope).astype(jnp.bfloat16)
    up_grad = (hidden_grad * gelu_value).astype(jnp.bfloat16)
    normed_grad = dot_transposed(gate_grad, gate_weight) + dot_transposed(up_grad, up_weight)
    weighted_in = input_gain * normed_grad
    cross_in = lax.optimization_barrier(jnp.mean(clean_rows * weighted_in, axis=1, keepdims=True))
    site_grad = (grad_rows + in_scale * weighted_in - clean_rows * in_scale * in_scale * in_scale * cross_in).astype(jnp.bfloat16)
    centered_clean = (clean_rows - decoder_bias).astype(jnp.bfloat16)
    centered_patch = (patch_stream.astype(jnp.float32) - decoder_bias).astype(jnp.bfloat16)
    block_width = LAT_DEV * N_MP
    targets = patch_positions + SEQ * jnp.arange(SEQS, dtype=jnp.int32)[:, None]

    def one_block(index):
        begin = (index * block_width).astype(jnp.int32)
        encoder_part = lax.dynamic_slice_in_dim(encoder_weight, begin, block_width, 1)
        bias_part = lax.dynamic_slice_in_dim(encoder_bias, begin, block_width, 0)
        decoder_part = lax.dynamic_slice_in_dim(decoder_weight, begin, block_width, 0)
        feature_clean = jnp.maximum(jnp.dot(centered_clean, encoder_part, preferred_element_type=jnp.float32) + bias_part, 0.0)
        feature_patch = jnp.maximum(jnp.dot(centered_patch, encoder_part, preferred_element_type=jnp.float32) + bias_part, 0.0)
        latent_grad = dot_transposed(site_grad, decoder_part)
        contribution = (feature_patch - feature_clean) * latent_grad
        totals = lax.optimization_barrier(jnp.sum(contribution.reshape(SEQS, SEQ, block_width), axis=1))
        picked = contribution[targets]
        return (totals, picked)
    totals, picked = lax.map(one_block, jnp.arange(N_LATENT, dtype=jnp.int32))
    latent_effects = jnp.transpose(totals, (1, 0, 2)).reshape(SEQS, LATENTS)
    position_effects = jnp.transpose(picked, (1, 2, 0, 3)).reshape(SEQS, P_SIZE, LATENTS)
    return (layer_output, latent_effects, position_effects)
```

```python
import jax
import jax.numpy as jnp
from jax import lax
from jax.sharding import PartitionSpec as P


epsilon = 1e-06
tanh_scale = 0.7978845608028654
cubic_term = 0.044715
LANES = 128
f32 = jnp.float32
bf16 = jnp.bfloat16


def gelu_parts(gate_sum):
    inner = tanh_scale * (gate_sum + cubic_term * gate_sum * gate_sum * gate_sum)
    tangent = jnp.tanh(inner)
    gelu_value = 0.5 * gate_sum * (1.0 + tangent)
    gelu_slope = 0.5 * (1.0 + tangent) + 0.5 * gate_sum * (1.0 - tangent * tangent) * tanh_scale * (
        1.0 + 3.0 * cubic_term * gate_sum * gate_sum
    )
    return (gelu_value, gelu_slope)


def dot(left, right):
    return jnp.dot(left, right, preferred_element_type=f32)


def dot_transposed(left, right):
    return lax.dot_general(left, right, (((1,), (1,)), ((), ())), preferred_element_type=f32)


def swap(value, axis, distance):
    count = lax.axis_size(axis)
    return lax.ppermute(value, axis, [(i, i ^ distance) for i in range(count)])


def split_columns(columns):
    rows = columns[0].shape[0]
    lane = lax.broadcasted_iota(jnp.int32, (rows, LANES), 1)
    block = jnp.zeros((rows, LANES), f32)
    for index, column in enumerate(columns):
        high = lax.reduce_precision(column, 8, 7)
        rest = column - high
        middle = lax.reduce_precision(rest, 8, 7)
        for part, piece in enumerate((high, middle, rest - middle)):
            block = jnp.where(lane == 3 * index + part, piece, block)
    return block.astype(bf16)


def join_columns(block, count):
    lane = lax.broadcasted_iota(jnp.int32, block.shape, 1)
    wide = block.astype(f32)
    return [
        jnp.sum(jnp.where(lane // 3 == index, wide, 0.0), axis=1, keepdims=True)
        for index in range(count)
    ]


def scatter_mp(partial):
    count = lax.axis_size("mp")
    rows = partial.shape[0] // count
    got = []
    for m in range(1, count):
        got.append(swap(partial[m * rows : (m + 1) * rows], "mp", m))
    return got


def gather_mp(block):
    blocks = [block]
    for m in range(1, lax.axis_size("mp")):
        blocks.append(swap(block, "mp", m))
    return jnp.concatenate(blocks, axis=0)


def reduce_latent(partial, extra):
    count = lax.axis_size("latent")
    side = lax.axis_index("latent") % 2 == 0
    half = partial.shape[0] // 2
    width = partial.shape[1]

    def pack(main, column):
        return main if column is None else jnp.concatenate([main, split_columns([column])], axis=1)

    def add(main, column, got):
        total = (main.astype(f32) + got[:, :width].astype(f32)).astype(bf16)
        return total, None if column is None else column + join_columns(got[:, width:], 1)[0]

    def pick(value, first):
        return jnp.where(first, value[:half], value[half:])

    main, column = pick(partial, side), None if extra is None else pick(extra, side)
    sent = pack(pick(partial, ~side), None if extra is None else pick(extra, ~side))
    got = swap(sent, "latent", 1)
    main, column = add(main, column, got)
    distances = [1 << bit for bit in range(1, count.bit_length() - 1)]
    quarter = half // 2
    done = []
    for lower, order in ((0, distances), (quarter, distances[::-1])):
        done.append(
            [main[lower : lower + quarter], None if column is None else column[lower : lower + quarter], order]
        )
    for step in range(len(distances)):
        got = [swap(pack(m, c), "latent", order[step]) for m, c, order in done]
        done = [[*add(m, c, g), order] for (m, c, order), g in zip(done, got)]
    main = jnp.concatenate([d[0] for d in done], axis=0)
    column = None if extra is None else jnp.concatenate([d[1] for d in done], axis=0)
    other = swap(pack(main, column), "latent", 1)
    low = jnp.where(side, main, other[:, :width])
    high = jnp.where(side, other[:, :width], main)
    total = jnp.concatenate([low, high], axis=0)
    if extra is None:
        return total, None
    far = join_columns(other[:, width:], 1)[0]
    return total, jnp.concatenate([jnp.where(side, column, far), jnp.where(side, far, column)], axis=0)


def program(
    clean_stream,
    patch_stream,
    output_grad,
    input_gain,
    gate_weight,
    up_weight,
    down_weight,
    output_gain,
    encoder_weight,
    encoder_bias,
    decoder_weight,
    decoder_bias,
    patch_positions,
):
    mp_count = lax.axis_size("mp")
    mp_index = lax.axis_index("mp")
    latent_index = lax.axis_index("latent")
    local_rows = clean_stream.shape[0]
    model_width = clean_stream.shape[1] * mp_count
    hidden_width = gate_weight.shape[1]
    tokens = local_rows * lax.axis_size("latent")
    rows = tokens // mp_count

    def by_distance(whole):
        return jnp.concatenate(
            [lax.dynamic_slice_in_dim(whole, (mp_index ^ m) * rows, rows, 0) for m in range(mp_count)], axis=0
        )

    clean = by_distance(lax.all_gather(clean_stream, "latent", axis=0, tiled=True))
    clean_rows = clean.astype(f32)
    square_part = jnp.sum(clean_rows * clean_rows, axis=1, keepdims=True)
    scaled = (clean_rows * input_gain).astype(bf16)
    gate_part = dot(scaled, gate_weight)
    up_part = dot(scaled, up_weight)
    sent = jnp.concatenate(
        [gate_part.astype(bf16), up_part.astype(bf16), split_columns([square_part])], axis=1
    )
    got = scatter_mp(sent)

    other_rows = jnp.concatenate([output_grad, patch_stream], axis=0)
    other_rows, _ = lax.optimization_barrier((other_rows, sent))
    others = lax.all_gather(other_rows, "latent", axis=0)
    got, others = lax.optimization_barrier((got, others))
    grad = by_distance(others[:, :local_rows].reshape(tokens, -1))
    patch = by_distance(others[:, local_rows:].reshape(tokens, -1))

    def total(part, pieces, begin):
        end = begin + part.shape[1]
        value = part[:rows]
        for piece in pieces:
            value = value + piece[:, begin:end].astype(f32)
        return value

    square_in = square_part[:rows]
    for piece in got:
        square_in = square_in + join_columns(piece[:, 2 * hidden_width :], 1)[0]
    in_scale = lax.rsqrt(square_in / model_width + epsilon)
    gate_sum = total(gate_part, got, 0) * in_scale
    up_sum = total(up_part, got, hidden_width) * in_scale
    gelu_value, gelu_slope = gelu_parts(gate_sum)
    gate_factor = up_sum * gelu_slope
    hidden = (gelu_value * up_sum).astype(bf16)
    radial = gate_factor * gate_sum + gelu_value * up_sum
    hidden_all = gather_mp(hidden)

    grad_rows = grad.astype(f32)
    weighted_out = output_gain * grad_rows
    linear_part = dot_transposed(weighted_out.astype(bf16), down_weight)
    linear_sent = linear_part.astype(bf16)
    encode_clean = dot((clean_rows - decoder_bias).astype(bf16), encoder_weight)
    encode_patch = dot((patch.astype(f32) - decoder_bias).astype(bf16), encoder_weight)
    clean_sent, patch_sent = encode_clean.astype(bf16), encode_patch.astype(bf16)
    linear_sent, clean_sent, hidden_all = lax.optimization_barrier((linear_sent, clean_sent, hidden_all))
    linear_got = scatter_mp(linear_sent)
    clean_got = scatter_mp(clean_sent)

    mlp_part = dot(hidden_all, down_weight).astype(bf16)
    mlp_out, _ = reduce_latent(mlp_part, None)
    mlp_rows = mlp_out.astype(f32)
    square_out = jnp.sum(mlp_rows * mlp_rows, axis=1, keepdims=True)
    cross_out = jnp.sum(mlp_rows * weighted_out, axis=1, keepdims=True)
    back_part = dot_transposed(mlp_out, down_weight)
    back_got = scatter_mp(jnp.concatenate([back_part.astype(bf16), split_columns([square_out, cross_out])], axis=1))
    square_own, cross_own = square_out[:rows], cross_out[:rows]
    for piece in back_got:
        square_piece, cross_piece = join_columns(piece[:, hidden_width:], 2)
        square_own, cross_own = square_own + square_piece, cross_own + cross_piece
    out_scale = lax.rsqrt(square_own / model_width + epsilon)
    hidden_grad = out_scale * total(linear_part, linear_got, 0) - (
        out_scale * out_scale * out_scale * (cross_own / model_width)
    ) * total(back_part, back_got, 0)
    gate_grad = (hidden_grad * gate_factor).astype(bf16)
    up_grad = (hidden_grad * gelu_value).astype(bf16)
    cross_in = jnp.sum(hidden_grad * radial, axis=1, keepdims=True)
    grads = gather_mp(jnp.concatenate([gate_grad, up_grad, split_columns([cross_in, in_scale, out_scale])], axis=1))
    cross_in, in_scale, out_scale = join_columns(grads[:, 2 * hidden_width :], 3)

    own_row = latent_index * local_rows
    own_row = (mp_index ^ (own_row // rows)) * rows + own_row % rows
    own = lambda value: lax.dynamic_slice_in_dim(value, own_row, local_rows, 0)
    block_rows = (
        clean_stream.astype(f32) + own(mlp_out).astype(f32) * own(out_scale) * output_gain
    ).astype(bf16)

    patch_sent, grads = lax.optimization_barrier((patch_sent, grads))
    patch_got = scatter_mp(patch_sent)
    latents = encoder_weight.shape[1]
    feature_delta = jnp.maximum(total(encode_patch, patch_got, 0) + encoder_bias, 0.0) - jnp.maximum(
        total(encode_clean, clean_got, 0) + encoder_bias, 0.0
    )
    feature_delta = gather_mp(feature_delta.astype(bf16)).astype(f32)

    normed_part = dot_transposed(grads[:, :hidden_width], gate_weight) + dot_transposed(
        grads[:, hidden_width : 2 * hidden_width], up_weight
    )
    normed_grad, cross_in = reduce_latent(normed_part.astype(bf16), cross_in)
    site_grad = (
        grad_rows
        + in_scale * (input_gain * normed_grad.astype(f32))
        - clean_rows * (in_scale * in_scale * (cross_in / model_width))
    ).astype(bf16)
    contribution = feature_delta * dot_transposed(site_grad, decoder_weight)

    sequences, picks = patch_positions.shape
    length = tokens // sequences
    targets = patch_positions + jnp.arange(sequences, dtype=jnp.int32)[:, None] * length
    targets = (mp_index ^ (targets // rows)) * rows + targets % rows
    token = (mp_index ^ (jnp.arange(tokens, dtype=jnp.int32) // rows)) * rows + jnp.arange(
        tokens, dtype=jnp.int32
    ) % rows
    inside = [(token // length == s)[:, None] for s in range(sequences)]
    chosen = [jnp.where(m, 1.0, 0.0).reshape(1, -1) for m in inside]
    chosen.append((targets.reshape(-1, 1) == jnp.arange(tokens, dtype=jnp.int32)[None]).astype(f32))
    effects = jnp.dot(jnp.concatenate(chosen, axis=0), contribution, precision=lax.Precision.HIGHEST)
    distance = 1
    while distance < mp_count:
        effects = effects + swap(effects, "mp", distance)
        distance *= 2
    return (block_rows, effects[:sequences], effects[sequences:].reshape(sequences, picks, latents))


def solution(mesh):
    in_specs = (
        P("latent", "mp"),
        P("latent", "mp"),
        P("latent", "mp"),
        P("mp"),
        P("mp", "latent"),
        P("mp", "latent"),
        P("latent", "mp"),
        P("mp"),
        P("mp", "latent"),
        P("latent"),
        P("latent", "mp"),
        P("mp"),
        P(),
    )
    out_specs = (P("latent", "mp"), P(None, "latent"), P(None, None, "latent"))
    return jax.shard_map(program, mesh=mesh, in_specs=in_specs, out_specs=out_specs, check_vma=False)
```

```python
import jax
import jax.numpy as jnp
from jax import lax
from jax.sharding import PartitionSpec as P


epsilon = 1e-06
tanh_scale = 0.7978845608028654
cubic_term = 0.044715
LANES = 128
f32 = jnp.float32
bf16 = jnp.bfloat16


def gelu_parts(gate_sum):
    inner = tanh_scale * (gate_sum + cubic_term * gate_sum * gate_sum * gate_sum)
    tangent = jnp.tanh(inner)
    gelu_value = 0.5 * gate_sum * (1.0 + tangent)
    gelu_slope = 0.5 * (1.0 + tangent) + 0.5 * gate_sum * (1.0 - tangent * tangent) * tanh_scale * (
        1.0 + 3.0 * cubic_term * gate_sum * gate_sum
    )
    return (gelu_value, gelu_slope)


def dot(left, right):
    return jnp.dot(left, right, preferred_element_type=f32)


def dot_transposed(left, right):
    return lax.dot_general(left, right, (((1,), (1,)), ((), ())), preferred_element_type=f32)


def swap(value, axis, distance):
    count = lax.axis_size(axis)
    return lax.ppermute(value, axis, [(i, i ^ distance) for i in range(count)])


def split_columns(columns):
    rows = columns[0].shape[0]
    lane = lax.broadcasted_iota(jnp.int32, (rows, LANES), 1)
    block = jnp.zeros((rows, LANES), f32)
    for index, column in enumerate(columns):
        high = lax.reduce_precision(column, 8, 7)
        rest = column - high
        middle = lax.reduce_precision(rest, 8, 7)
        for part, piece in enumerate((high, middle, rest - middle)):
            block = jnp.where(lane == 3 * index + part, piece, block)
    return block.astype(bf16)


def join_columns(block, count):
    lane = lax.broadcasted_iota(jnp.int32, block.shape, 1)
    wide = block.astype(f32)
    return [
        jnp.sum(jnp.where(lane // 3 == index, wide, 0.0), axis=1, keepdims=True)
        for index in range(count)
    ]


def send_mp(blocks):
    got = []
    for m in reversed(range(1, lax.axis_size("mp"))):
        got.append(swap(blocks[m - 1], "mp", m))
    return got


def gather_mp(block):
    blocks = [block]
    for m in reversed(range(1, lax.axis_size("mp"))):
        blocks.insert(1, swap(block, "mp", m))
    return jnp.concatenate(blocks, axis=0)


def reduce_latent(partial, extra, side):
    count = lax.axis_size("latent")
    half = partial.shape[0] // 2
    width = partial.shape[1]

    def pack(main, column):
        return main if column is None else jnp.concatenate([main, split_columns([column])], axis=1)

    def add(main, column, got):
        total = (main.astype(f32) + got[:, :width].astype(f32)).astype(bf16)
        return total, None if column is None else column + join_columns(got[:, width:], 1)[0]

    def pick(value, first):
        return jnp.where(first, value[:half], value[half:])

    main, column = pick(partial, side), None if extra is None else pick(extra, side)
    sent = pack(pick(partial, ~side), None if extra is None else pick(extra, ~side))
    got = swap(sent, "latent", 1)
    main, column = add(main, column, got)
    distances = [1 << bit for bit in range(1, count.bit_length() - 1)]
    quarter = half // 2
    done = []
    for lower, order in ((0, distances), (quarter, distances[::-1])):
        done.append(
            [main[lower : lower + quarter], None if column is None else column[lower : lower + quarter], order]
        )
    for step in range(len(distances)):
        got = [swap(pack(m, c), "latent", order[step]) for m, c, order in done]
        done = [[*add(m, c, g), order] for (m, c, order), g in zip(done, got)]
    main = jnp.concatenate([d[0] for d in done], axis=0)
    column = None if extra is None else jnp.concatenate([d[1] for d in done], axis=0)
    other = swap(pack(main, column), "latent", 1)
    low = jnp.where(side, main, other[:, :width])
    high = jnp.where(side, other[:, :width], main)
    total = jnp.concatenate([low, high], axis=0)
    if extra is None:
        return total, None
    far = join_columns(other[:, width:], 1)[0]
    return total, jnp.concatenate([jnp.where(side, column, far), jnp.where(side, far, column)], axis=0)


def program(
    clean_stream,
    patch_stream,
    output_grad,
    input_gain,
    gate_weight,
    up_weight,
    down_weight,
    output_gain,
    encoder_weight,
    encoder_bias,
    decoder_weight,
    decoder_bias,
    patch_positions,
):
    mp_count = lax.axis_size("mp")
    mp_index = lax.axis_index("mp")
    latent_index = lax.axis_index("latent")
    local_rows = clean_stream.shape[0]
    model_width = clean_stream.shape[1] * mp_count
    hidden_width = gate_weight.shape[1]
    tokens = local_rows * lax.axis_size("latent")
    rows = tokens // mp_count

    def total(own, pieces):
        for piece in pieces:
            own = own + piece.astype(f32)
        return own

    sequences, picks = patch_positions.shape
    length = tokens // sequences
    starts = [(mp_index ^ m) * rows for m in range(mp_count)]
    side = (latent_index & 1) == 0
    own_row = latent_index * local_rows
    own_row = (mp_index ^ lax.div(own_row, rows)) * rows + lax.rem(own_row, rows)
    streams = jnp.concatenate([clean_stream, output_grad, patch_stream], axis=1)
    starts, side, own_row, mp_index, streams = lax.optimization_barrier(
        (starts, side, own_row, mp_index, streams)
    )

    def block_of(value, distance):
        zero = jnp.zeros((), jnp.int32)
        return lax.dynamic_slice(
            value, (starts[distance], zero), (rows, value.shape[1]), allow_negative_indices=False
        )

    def blocks_of(value):
        return [block_of(value, m) for m in range(1, mp_count)]

    streams = lax.all_gather(streams, "latent", axis=0, tiled=True)
    width = clean_stream.shape[1]
    clean = streams[:, :width]
    clean_rows = clean.astype(f32)
    scaled = (clean_rows * input_gain).astype(bf16)
    gate_part = dot(scaled, gate_weight)
    square_part = jnp.sum(clean_rows * clean_rows, axis=1, keepdims=True)
    gate_sent = jnp.concatenate([gate_part.astype(bf16), split_columns([square_part])], axis=1)
    gate_got = send_mp(blocks_of(gate_sent))
    up_part = dot(scaled, up_weight)
    up_sent = up_part.astype(bf16)
    up_got = send_mp(blocks_of(up_sent))
    streams, patch_positions, mp_index, _ = lax.optimization_barrier(
        (streams, patch_positions, mp_index, up_sent)
    )
    place = jnp.arange(tokens, dtype=jnp.int32)
    token = (mp_index ^ lax.div(place, rows)) * rows + lax.rem(place, rows)
    targets = patch_positions + jnp.arange(sequences, dtype=jnp.int32)[:, None] * length
    inside = lax.div(token, length)[None] == jnp.arange(sequences, dtype=jnp.int32)[:, None]
    chosen = jnp.concatenate([inside, targets.reshape(-1, 1) == token[None]], axis=0).astype(f32)
    grad, patch = streams[:, width : 2 * width], streams[:, 2 * width :]

    square_in = block_of(square_part, 0)
    for piece in gate_got:
        square_in = square_in + join_columns(piece[:, hidden_width:], 1)[0]
    in_scale = lax.rsqrt(square_in / model_width + epsilon)
    gate_sum = total(block_of(gate_part, 0), [piece[:, :hidden_width] for piece in gate_got]) * in_scale
    up_sum = total(block_of(up_part, 0), up_got) * in_scale
    hidden = (gelu_parts(gate_sum)[0] * up_sum).astype(bf16)
    hidden_all = gather_mp(hidden)
    gate_sum, up_sum, _ = lax.optimization_barrier((gate_sum, up_sum, hidden))
    gelu_value, gelu_slope = gelu_parts(gate_sum)
    gate_factor = up_sum * gelu_slope
    radial = gate_factor * gate_sum + gelu_value * up_sum

    linear_part = dot_transposed((output_gain * grad.astype(f32)).astype(bf16), down_weight)
    linear_sent = linear_part.astype(bf16)
    linear_got = send_mp(blocks_of(linear_sent))

    encode_clean = dot((clean_rows - decoder_bias).astype(bf16), encoder_weight)
    encode_patch = dot((patch.astype(f32) - decoder_bias).astype(bf16), encoder_weight)
    encode_sent = [
        jnp.concatenate([block_of(encode_clean, m), block_of(encode_patch, m)], axis=0).astype(bf16)
        for m in range(1, mp_count)
    ]

    ordered = [jnp.concatenate([block_of(v, m) for m in range(mp_count)], axis=0) for v in (clean, grad)]
    clean_rows, grad_rows = (value.astype(f32) for value in lax.optimization_barrier(ordered))
    weighted_out = output_gain * grad_rows

    mlp_part = dot(hidden_all, down_weight).astype(bf16)
    mlp_out, _ = reduce_latent(mlp_part, None, side)
    mlp_rows = mlp_out.astype(f32)
    square_out = jnp.sum(mlp_rows * mlp_rows, axis=1, keepdims=True)
    cross_out = jnp.sum(mlp_rows * weighted_out, axis=1, keepdims=True)
    back_part = dot_transposed(mlp_out, down_weight)
    back_sent = jnp.concatenate([back_part.astype(bf16), split_columns([square_out, cross_out])], axis=1)
    back_got = send_mp([back_sent[m * rows : (m + 1) * rows] for m in range(1, mp_count)])
    square_own, cross_own = square_out[:rows], cross_out[:rows]
    for piece in back_got:
        square_piece, cross_piece = join_columns(piece[:, hidden_width:], 2)
        square_own, cross_own = square_own + square_piece, cross_own + cross_piece
    out_scale = lax.rsqrt(square_own / model_width + epsilon)
    hidden_grad = out_scale * total(block_of(linear_part, 0), linear_got) - (
        out_scale * out_scale * out_scale * (cross_own / model_width)
    ) * total(back_part[:rows], [piece[:, :hidden_width] for piece in back_got])
    gate_grad = (hidden_grad * gate_factor).astype(bf16)
    cross_in = jnp.sum(hidden_grad * radial, axis=1, keepdims=True)
    gate_grads = gather_mp(jnp.concatenate([gate_grad, split_columns([cross_in, in_scale, out_scale])], axis=1))
    up_grads = gather_mp((hidden_grad * gelu_value).astype(bf16))
    cross_in, in_scale, out_scale = join_columns(gate_grads[:, hidden_width:], 3)


    encode_got = send_mp(encode_sent)
    latents = encoder_weight.shape[1]
    own_sums = jnp.concatenate([block_of(encode_clean, 0), block_of(encode_patch, 0)], axis=0)
    feature = jnp.maximum(total(own_sums, encode_got) + encoder_bias, 0.0)
    feature_delta = gather_mp((feature[rows:] - feature[:rows]).astype(bf16)).astype(f32)

    gate_back = dot_transposed(gate_grads[:, :hidden_width], gate_weight)
    normed_part = dot_transposed(up_grads, up_weight) + gate_back
    normed_grad, cross_in = reduce_latent(normed_part.astype(bf16), cross_in, side)
    site_grad = (
        grad_rows
        + in_scale * (input_gain * normed_grad.astype(f32))
        - clean_rows * (in_scale * in_scale * (cross_in / model_width))
    ).astype(bf16)
    contribution = feature_delta * dot_transposed(site_grad, decoder_weight)

    effects = jnp.dot(chosen, contribution, precision=lax.Precision.HIGHEST)
    mlp_out, out_scale, effects = lax.optimization_barrier((mlp_out, out_scale, effects))

    def own(value):
        zero = jnp.zeros((), jnp.int32)
        return lax.dynamic_slice(
            value, (own_row, zero), (local_rows, value.shape[1]), allow_negative_indices=False
        )

    block_rows = (
        clean_stream.astype(f32) + own(mlp_out).astype(f32) * own(out_scale) * output_gain
    ).astype(bf16)
    terms = [effects] + [swap(effects, "mp", m) for m in range(1, mp_count)]
    while len(terms) > 1:
        terms = [left + right for left, right in zip(terms[::2], terms[1::2])]
    effects = terms[0]
    return (block_rows, effects[:sequences], effects[sequences:].reshape(sequences, picks, latents))


def solution(mesh):
    in_specs = (
        P("latent", "mp"),
        P("latent", "mp"),
        P("latent", "mp"),
        P("mp"),
        P("mp", "latent"),
        P("mp", "latent"),
        P("latent", "mp"),
        P("mp"),
        P("mp", "latent"),
        P("latent"),
        P("latent", "mp"),
        P("mp"),
        P(),
    )
    out_specs = (P("latent", "mp"), P(None, "latent"), P(None, None, "latent"))
    return jax.shard_map(program, mesh=mesh, in_specs=in_specs, out_specs=out_specs, check_vma=False)
```

```python
import jax
import jax.numpy as jnp
from jax import lax
from jax.experimental import pallas as pl
from jax.experimental.pallas import tpu as pltpu
from jax.sharding import PartitionSpec as P


epsilon = 1e-06
tanh_scale = 0.7978845608028654
cubic_term = 0.044715
LANES = 128
f32 = jnp.float32
bf16 = jnp.bfloat16


def gelu_parts(gate_sum):
    inner = tanh_scale * (gate_sum + cubic_term * gate_sum * gate_sum * gate_sum)
    tangent = jnp.tanh(inner)
    gelu_value = 0.5 * gate_sum * (1.0 + tangent)
    gelu_slope = 0.5 * (1.0 + tangent) + 0.5 * gate_sum * (1.0 - tangent * tangent) * tanh_scale * (
        1.0 + 3.0 * cubic_term * gate_sum * gate_sum
    )
    return (gelu_value, gelu_slope)


def dot(left, right):
    return jnp.dot(left, right, preferred_element_type=f32)


def dot_transposed(left, right):
    return lax.dot_general(left, right, (((1,), (1,)), ((), ())), preferred_element_type=f32)


def swap(value, axis, distance):
    count = lax.axis_size(axis)
    return lax.ppermute(value, axis, [(i, i ^ distance) for i in range(count)])


def split_columns(columns):
    rows = columns[0].shape[0]
    lane = lax.broadcasted_iota(jnp.int32, (rows, LANES), 1)
    block = jnp.zeros((rows, LANES), f32)
    for index, column in enumerate(columns):
        high = lax.reduce_precision(column, 8, 7)
        rest = column - high
        middle = lax.reduce_precision(rest, 8, 7)
        for part, piece in enumerate((high, middle, rest - middle)):
            block = jnp.where(lane == 3 * index + part, piece, block)
    return block.astype(bf16)


def join_columns(block, count):
    lane = lax.broadcasted_iota(jnp.int32, block.shape, 1)
    wide = block.astype(f32)
    return [
        jnp.sum(jnp.where(lane // 3 == index, wide, 0.0), axis=1, keepdims=True)
        for index in range(count)
    ]


def handed_on(source_ref, target_ref):
    target_ref[...] = source_ref[...]


def before_gather(value):
    vmem = pl.BlockSpec(memory_space=pltpu.VMEM)
    return pl.pallas_call(
        handed_on,
        out_shape=jax.ShapeDtypeStruct(value.shape, value.dtype),
        in_specs=[vmem],
        out_specs=vmem,
        compiler_params=pltpu.CompilerParams(vmem_limit_bytes=2 << 20),
        cost_estimate=pl.CostEstimate(flops=1 << 34, bytes_accessed=32 << 20, transcendentals=0),
        name="before_gather",
    )(value)


def send_mp(blocks):
    got = []
    for m in reversed(range(1, lax.axis_size("mp"))):
        got.append(swap(blocks[m - 1], "mp", m))
    return got


def gather_mp(block):
    blocks = [block]
    for m in reversed(range(1, lax.axis_size("mp"))):
        blocks.insert(1, swap(block, "mp", m))
    return jnp.concatenate(blocks, axis=0)


def relay_mp(block):
    if lax.axis_size("mp") != 4:
        return gather_mp(block)

    def send(value, pairs):
        return lax.ppermute(value, "mp", pairs)

    rows = block.shape[0]
    outer = send(block, [(0, 2), (3, 1)])
    inner = send(block, [(1, 2), (2, 1)])
    near = send(block, [(i, i ^ 1) for i in range(4)])
    passed = send(jnp.concatenate([inner, outer], axis=0), [(2, 3), (1, 0)])
    return jnp.concatenate([block, near, outer + passed[:rows], inner + passed[rows:]], axis=0)


def reduce_latent(partial, extra, sides):
    count = lax.axis_size("latent")
    side, other_side = sides
    half = partial.shape[0] // 2
    width = partial.shape[1]

    def pack(main, column):
        return main if column is None else jnp.concatenate([main, split_columns([column])], axis=1)

    def add(main, column, got):
        total = (main.astype(f32) + got[:, :width].astype(f32)).astype(bf16)
        return total, None if column is None else column + join_columns(got[:, width:], 1)[0]

    def pick(value, first):
        return jnp.where(first, value[:half], value[half:])

    main, column = pick(partial, side), None if extra is None else pick(extra, side)
    sent = pack(pick(partial, other_side), None if extra is None else pick(extra, other_side))
    got = swap(sent, "latent", 1)
    main, column = add(main, column, got)
    bits = [1 << bit for bit in range(1, count.bit_length() - 1)]
    for step in range(0, len(bits), 2):
        group = bits[step : step + 2]
        terms = [(main.astype(f32), column)]
        for distance in [group[0]] if len(group) == 1 else [group[0], group[1], sum(group)]:
            got = swap(pack(main, column), "latent", distance)
            far = None if column is None else join_columns(got[:, width:], 1)[0]
            terms.append((got[:, :width].astype(f32), far))
        while len(terms) > 1:
            terms = [
                (left[0] + right[0], None if column is None else left[1] + right[1])
                for left, right in zip(terms[::2], terms[1::2])
            ]
        main, column = terms[0][0].astype(bf16), terms[0][1]
    other = swap(pack(main, column), "latent", 1)
    low = jnp.where(side, main, other[:, :width])
    high = jnp.where(side, other[:, :width], main)
    total = jnp.concatenate([low, high], axis=0)
    if extra is None:
        return total, None
    far = join_columns(other[:, width:], 1)[0]
    return total, jnp.concatenate([jnp.where(side, column, far), jnp.where(side, far, column)], axis=0)


def program(
    clean_stream,
    patch_stream,
    output_grad,
    input_gain,
    gate_weight,
    up_weight,
    down_weight,
    output_gain,
    encoder_weight,
    encoder_bias,
    decoder_weight,
    decoder_bias,
    patch_positions,
):
    mp_count = lax.axis_size("mp")
    mp_index = lax.axis_index("mp")
    latent_index = lax.axis_index("latent")
    local_rows = clean_stream.shape[0]
    model_width = clean_stream.shape[1] * mp_count
    hidden_width = gate_weight.shape[1]
    tokens = local_rows * lax.axis_size("latent")
    rows = tokens // mp_count

    def total(own, pieces):
        for piece in pieces:
            own = own + piece.astype(f32)
        return own

    sequences, picks = patch_positions.shape
    length = tokens // sequences
    starts = [(mp_index ^ m) * rows for m in range(mp_count)]
    sides = ((latent_index & 1) == 0, (latent_index & 1) == 1)
    own_row = latent_index * local_rows
    own_row = (mp_index ^ lax.div(own_row, rows)) * rows + lax.rem(own_row, rows)
    streams = jnp.concatenate([clean_stream, output_grad, patch_stream], axis=1)
    starts, sides, own_row, mp_index, streams = lax.optimization_barrier(
        (starts, sides, own_row, mp_index, streams)
    )

    def block_of(value, distance):
        zero = jnp.zeros((), jnp.int32)
        return lax.dynamic_slice(
            value, (starts[distance], zero), (rows, value.shape[1]), allow_negative_indices=False
        )

    def blocks_of(value):
        return [block_of(value, m) for m in range(1, mp_count)]

    streams = lax.all_gather(before_gather(streams), "latent", axis=0, tiled=True)
    width = clean_stream.shape[1]
    clean = streams[:, :width]
    clean_rows = clean.astype(f32)
    scaled = (clean_rows * input_gain).astype(bf16)
    gate_part = dot(scaled, gate_weight)
    square_part = jnp.sum(clean_rows * clean_rows, axis=1, keepdims=True)
    gate_sent = jnp.concatenate([gate_part.astype(bf16), split_columns([square_part])], axis=1)
    gate_got = send_mp(blocks_of(gate_sent))
    up_part = dot(scaled, up_weight)
    up_sent = up_part.astype(bf16)
    up_got = send_mp(blocks_of(up_sent))
    streams, patch_positions, mp_index, _ = lax.optimization_barrier(
        (streams, patch_positions, mp_index, up_sent)
    )
    place = jnp.arange(tokens, dtype=jnp.int32)
    token = (mp_index ^ lax.div(place, rows)) * rows + lax.rem(place, rows)
    targets = patch_positions + jnp.arange(sequences, dtype=jnp.int32)[:, None] * length
    inside = lax.div(token, length)[None] == jnp.arange(sequences, dtype=jnp.int32)[:, None]
    chosen = jnp.concatenate([inside, targets.reshape(-1, 1) == token[None]], axis=0).astype(f32)
    grad, patch = streams[:, width : 2 * width], streams[:, 2 * width :]

    square_in = block_of(square_part, 0)
    for piece in gate_got:
        square_in = square_in + join_columns(piece[:, hidden_width:], 1)[0]
    in_scale = lax.rsqrt(square_in / model_width + epsilon)
    gate_sum = total(block_of(gate_part, 0), [piece[:, :hidden_width] for piece in gate_got]) * in_scale
    up_sum = total(block_of(up_part, 0), up_got) * in_scale
    hidden = (gelu_parts(gate_sum)[0] * up_sum).astype(bf16)
    hidden_all = gather_mp(hidden)
    gate_sum, up_sum, _ = lax.optimization_barrier((gate_sum, up_sum, hidden))
    gelu_value, gelu_slope = gelu_parts(gate_sum)
    gate_factor = up_sum * gelu_slope
    radial = gate_factor * gate_sum + gelu_value * up_sum

    linear_part = dot_transposed((output_gain * grad.astype(f32)).astype(bf16), down_weight)
    linear_sent = linear_part.astype(bf16)
    encode_clean = dot((clean_rows - decoder_bias).astype(bf16), encoder_weight)
    clean_sent = encode_clean.astype(bf16)
    linear_got = send_mp([jnp.concatenate(pair, axis=1) for pair in zip(blocks_of(linear_sent), blocks_of(clean_sent))])
    clean_got = [piece[:, hidden_width:] for piece in linear_got]
    linear_got = [piece[:, :hidden_width] for piece in linear_got]
    encode_patch = dot((patch.astype(f32) - decoder_bias).astype(bf16), encoder_weight)
    patch_sent = encode_patch.astype(bf16)

    ordered = [jnp.concatenate([block_of(v, m) for m in range(mp_count)], axis=0) for v in (clean, grad)]
    clean_rows, grad_rows = (value.astype(f32) for value in lax.optimization_barrier(ordered))
    weighted_out = output_gain * grad_rows

    mlp_part = dot(hidden_all, down_weight).astype(bf16)
    mlp_out, _ = reduce_latent(mlp_part, None, sides)
    mlp_rows = mlp_out.astype(f32)
    square_out = jnp.sum(mlp_rows * mlp_rows, axis=1, keepdims=True)
    cross_out = jnp.sum(mlp_rows * weighted_out, axis=1, keepdims=True)
    back_part = dot_transposed(mlp_out, down_weight)
    back_sent = jnp.concatenate([back_part.astype(bf16), split_columns([square_out, cross_out])], axis=1)
    back_got = send_mp([back_sent[m * rows : (m + 1) * rows] for m in range(1, mp_count)])
    square_own, cross_own = square_out[:rows], cross_out[:rows]
    for piece in back_got:
        square_piece, cross_piece = join_columns(piece[:, hidden_width:], 2)
        square_own, cross_own = square_own + square_piece, cross_own + cross_piece
    out_scale = lax.rsqrt(square_own / model_width + epsilon)
    hidden_grad = out_scale * total(block_of(linear_part, 0), linear_got) - (
        out_scale * out_scale * out_scale * (cross_own / model_width)
    ) * total(back_part[:rows], [piece[:, :hidden_width] for piece in back_got])
    up_grads = relay_mp((hidden_grad * gelu_value).astype(bf16))
    gate_grad = (hidden_grad * gate_factor).astype(bf16)
    cross_in = jnp.sum(hidden_grad * radial, axis=1, keepdims=True)
    gate_grads = gather_mp(jnp.concatenate([gate_grad, split_columns([cross_in, in_scale, out_scale])], axis=1))
    cross_in, in_scale, out_scale = join_columns(gate_grads[:, hidden_width:], 3)


    patch_got = send_mp(blocks_of(patch_sent))
    latents = encoder_weight.shape[1]
    feature_clean = jnp.maximum(total(block_of(encode_clean, 0), clean_got) + encoder_bias, 0.0)
    feature_patch = jnp.maximum(total(block_of(encode_patch, 0), patch_got) + encoder_bias, 0.0)
    feature_delta = gather_mp((feature_patch - feature_clean).astype(bf16)).astype(f32)

    gate_back = dot_transposed(gate_grads[:, :hidden_width], gate_weight)
    normed_part = dot_transposed(up_grads, up_weight) + gate_back
    normed_grad, cross_in = reduce_latent(normed_part.astype(bf16), cross_in, sides)
    site_grad = (
        grad_rows
        + in_scale * (input_gain * normed_grad.astype(f32))
        - clean_rows * (in_scale * in_scale * (cross_in / model_width))
    ).astype(bf16)
    contribution = feature_delta * dot_transposed(site_grad, decoder_weight)

    effects = jnp.dot(chosen, contribution, precision=lax.Precision.HIGHEST)
    mlp_out, out_scale, effects = lax.optimization_barrier((mlp_out, out_scale, effects))

    def own(value):
        zero = jnp.zeros((), jnp.int32)
        return lax.dynamic_slice(
            value, (own_row, zero), (local_rows, value.shape[1]), allow_negative_indices=False
        )

    block_rows = (
        clean_stream.astype(f32) + own(mlp_out).astype(f32) * own(out_scale) * output_gain
    ).astype(bf16)
    terms = [effects] + [swap(effects, "mp", m) for m in range(1, mp_count)]
    while len(terms) > 1:
        terms = [left + right for left, right in zip(terms[::2], terms[1::2])]
    effects = terms[0]
    return (block_rows, effects[:sequences], effects[sequences:].reshape(sequences, picks, latents))


def solution(mesh):
    in_specs = (
        P("latent", "mp"),
        P("latent", "mp"),
        P("latent", "mp"),
        P("mp"),
        P("mp", "latent"),
        P("mp", "latent"),
        P("latent", "mp"),
        P("mp"),
        P("mp", "latent"),
        P("latent"),
        P("latent", "mp"),
        P("mp"),
        P(),
    )
    out_specs = (P("latent", "mp"), P(None, "latent"), P(None, None, "latent"))
    return jax.shard_map(program, mesh=mesh, in_specs=in_specs, out_specs=out_specs, check_vma=False)
```

```python
import jax
import jax.numpy as jnp
from jax import lax
from jax.experimental import pallas as pl
from jax.experimental.pallas import tpu as pltpu
from jax.sharding import PartitionSpec as P


epsilon = 1e-06
tanh_scale = 0.7978845608028654
cubic_term = 0.044715
LANES = 128
f32 = jnp.float32
bf16 = jnp.bfloat16


def gelu_parts(gate_sum):
    inner = tanh_scale * (gate_sum + cubic_term * gate_sum * gate_sum * gate_sum)
    tangent = jnp.tanh(inner)
    gelu_value = 0.5 * gate_sum * (1.0 + tangent)
    gelu_slope = 0.5 * (1.0 + tangent) + 0.5 * gate_sum * (1.0 - tangent * tangent) * tanh_scale * (
        1.0 + 3.0 * cubic_term * gate_sum * gate_sum
    )
    return (gelu_value, gelu_slope)


def dot(left, right):
    return jnp.dot(left, right, preferred_element_type=f32)


def dot_transposed(left, right):
    return lax.dot_general(left, right, (((1,), (1,)), ((), ())), preferred_element_type=f32)


def swap(value, axis, distance):
    count = lax.axis_size(axis)
    return lax.ppermute(value, axis, [(i, i ^ distance) for i in range(count)])


def split_columns(columns):
    rows = columns[0].shape[0]
    lane = lax.broadcasted_iota(jnp.int32, (rows, LANES), 1)
    block = jnp.zeros((rows, LANES), f32)
    for index, column in enumerate(columns):
        high = lax.reduce_precision(column, 8, 7)
        rest = column - high
        middle = lax.reduce_precision(rest, 8, 7)
        for part, piece in enumerate((high, middle, rest - middle)):
            block = jnp.where(lane == 3 * index + part, piece, block)
    return block.astype(bf16)


def join_columns(block, count):
    lane = lax.broadcasted_iota(jnp.int32, block.shape, 1)
    wide = block.astype(f32)
    return [
        jnp.sum(jnp.where(lane // 3 == index, wide, 0.0), axis=1, keepdims=True)
        for index in range(count)
    ]


def handed_on(source_ref, target_ref):
    target_ref[...] = source_ref[...]


def before_gather(value):
    vmem = pl.BlockSpec(memory_space=pltpu.VMEM)
    return pl.pallas_call(
        handed_on,
        out_shape=jax.ShapeDtypeStruct(value.shape, value.dtype),
        in_specs=[vmem],
        out_specs=vmem,
        compiler_params=pltpu.CompilerParams(vmem_limit_bytes=2 << 20),
        cost_estimate=pl.CostEstimate(flops=1 << 34, bytes_accessed=32 << 20, transcendentals=0),
        name="before_gather",
    )(value)


def send_mp(blocks):
    got = []
    for m in reversed(range(1, lax.axis_size("mp"))):
        got.append(swap(blocks[m - 1], "mp", m))
    return got


def relay_sums(blocks):
    if lax.axis_size("mp") != 4:
        return send_mp(blocks)

    def send(value, pairs):
        return lax.ppermute(value, "mp", pairs)

    def join(left, right):
        return (left.astype(f32) + right.astype(f32)).astype(bf16)

    far = jnp.concatenate(blocks[1:], axis=0)
    rows = far.shape[0] // 2
    got = send(far, [(0, 1), (3, 2)])
    near = send(blocks[0], [(i, i ^ 1) for i in range(4)])
    middle = send(join(far[rows:], got[:rows]), [(1, 2), (2, 1)])
    outer = send(join(far[:rows], got[rows:]), [(1, 3), (2, 0)])
    return [near, middle, outer]


def gather_mp(block):
    blocks = [block]
    for m in reversed(range(1, lax.axis_size("mp"))):
        blocks.insert(1, swap(block, "mp", m))
    return jnp.concatenate(blocks, axis=0)


def relay_mp(block):
    if lax.axis_size("mp") != 4:
        return gather_mp(block)

    def send(value, pairs):
        return lax.ppermute(value, "mp", pairs)

    rows = block.shape[0]
    outer = send(block, [(0, 2), (3, 1)])
    inner = send(block, [(1, 2), (2, 1)])
    near = send(block, [(i, i ^ 1) for i in range(4)])
    passed = send(jnp.concatenate([inner, outer], axis=0), [(2, 3), (1, 0)])
    return jnp.concatenate([block, near, outer + passed[:rows], inner + passed[rows:]], axis=0)


def reduce_latent(partial, extra, sides):
    count = lax.axis_size("latent")
    side, other_side = sides
    half = partial.shape[0] // 2
    width = partial.shape[1]

    def pack(main, column):
        return main if column is None else jnp.concatenate([main, split_columns([column])], axis=1)

    def add(main, column, got):
        total = (main.astype(f32) + got[:, :width].astype(f32)).astype(bf16)
        return total, None if column is None else column + join_columns(got[:, width:], 1)[0]

    def pick(value, first):
        return jnp.where(first, value[:half], value[half:])

    main, column = pick(partial, side), None if extra is None else pick(extra, side)
    sent = pack(pick(partial, other_side), None if extra is None else pick(extra, other_side))
    got = swap(sent, "latent", 1)
    main, column = add(main, column, got)
    bits = [1 << bit for bit in range(1, count.bit_length() - 1)]
    for step in range(0, len(bits), 2):
        group = bits[step : step + 2]
        terms = [(main.astype(f32), column)]
        for distance in [group[0]] if len(group) == 1 else [group[0], group[1], sum(group)]:
            got = swap(pack(main, column), "latent", distance)
            far = None if column is None else join_columns(got[:, width:], 1)[0]
            terms.append((got[:, :width].astype(f32), far))
        while len(terms) > 1:
            terms = [
                (left[0] + right[0], None if column is None else left[1] + right[1])
                for left, right in zip(terms[::2], terms[1::2])
            ]
        main, column = terms[0][0].astype(bf16), terms[0][1]
    other = swap(pack(main, column), "latent", 1)
    low = jnp.where(side, main, other[:, :width])
    high = jnp.where(side, other[:, :width], main)
    total = jnp.concatenate([low, high], axis=0)
    if extra is None:
        return total, None
    far = join_columns(other[:, width:], 1)[0]
    return total, jnp.concatenate([jnp.where(side, column, far), jnp.where(side, far, column)], axis=0)


def program(
    clean_stream,
    patch_stream,
    output_grad,
    input_gain,
    gate_weight,
    up_weight,
    down_weight,
    output_gain,
    encoder_weight,
    encoder_bias,
    decoder_weight,
    decoder_bias,
    patch_positions,
):
    mp_count = lax.axis_size("mp")
    mp_index = lax.axis_index("mp")
    latent_index = lax.axis_index("latent")
    local_rows = clean_stream.shape[0]
    model_width = clean_stream.shape[1] * mp_count
    hidden_width = gate_weight.shape[1]
    tokens = local_rows * lax.axis_size("latent")
    rows = tokens // mp_count

    def total(own, pieces):
        for piece in pieces:
            own = own + piece.astype(f32)
        return own

    sequences, picks = patch_positions.shape
    length = tokens // sequences
    starts = [(mp_index ^ m) * rows for m in range(mp_count)]
    sides = ((latent_index & 1) == 0, (latent_index & 1) == 1)
    own_row = latent_index * local_rows
    own_row = (mp_index ^ lax.div(own_row, rows)) * rows + lax.rem(own_row, rows)
    streams = jnp.concatenate([clean_stream, output_grad, patch_stream], axis=1)
    starts, sides, own_row, mp_index, streams = lax.optimization_barrier(
        (starts, sides, own_row, mp_index, streams)
    )

    def block_of(value, distance):
        zero = jnp.zeros((), jnp.int32)
        return lax.dynamic_slice(
            value, (starts[distance], zero), (rows, value.shape[1]), allow_negative_indices=False
        )

    def blocks_of(value):
        return [block_of(value, m) for m in range(1, mp_count)]

    streams = lax.all_gather(before_gather(streams), "latent", axis=0, tiled=True)
    width = clean_stream.shape[1]
    clean = streams[:, :width]
    clean_rows = clean.astype(f32)
    scaled = (clean_rows * input_gain).astype(bf16)
    up_part = dot(scaled, up_weight)
    up_got = relay_sums(blocks_of(up_part.astype(bf16)))
    gate_part = dot(scaled, gate_weight)
    square_part = jnp.sum(clean_rows * clean_rows, axis=1, keepdims=True)
    gate_sent = jnp.concatenate([gate_part.astype(bf16), split_columns([square_part])], axis=1)
    gate_got = send_mp(blocks_of(gate_sent))
    streams, patch_positions, mp_index, _ = lax.optimization_barrier(
        (streams, patch_positions, mp_index, gate_sent)
    )
    place = jnp.arange(tokens, dtype=jnp.int32)
    token = (mp_index ^ lax.div(place, rows)) * rows + lax.rem(place, rows)
    targets = patch_positions + jnp.arange(sequences, dtype=jnp.int32)[:, None] * length
    inside = lax.div(token, length)[None] == jnp.arange(sequences, dtype=jnp.int32)[:, None]
    chosen = jnp.concatenate([inside, targets.reshape(-1, 1) == token[None]], axis=0).astype(f32)
    grad, patch = streams[:, width : 2 * width], streams[:, 2 * width :]

    square_in = block_of(square_part, 0)
    for piece in gate_got:
        square_in = square_in + join_columns(piece[:, hidden_width:], 1)[0]
    in_scale = lax.rsqrt(square_in / model_width + epsilon)
    gate_sum = total(block_of(gate_part, 0), [piece[:, :hidden_width] for piece in gate_got]) * in_scale
    up_sum = total(block_of(up_part, 0), up_got) * in_scale
    hidden = (gelu_parts(gate_sum)[0] * up_sum).astype(bf16)
    hidden_all = gather_mp(hidden)
    gate_sum, up_sum, _ = lax.optimization_barrier((gate_sum, up_sum, hidden))
    gelu_value, gelu_slope = gelu_parts(gate_sum)
    gate_factor = up_sum * gelu_slope
    radial = gate_factor * gate_sum + gelu_value * up_sum

    linear_part = dot_transposed((output_gain * grad.astype(f32)).astype(bf16), down_weight)
    linear_sent = linear_part.astype(bf16)
    encode_clean = dot((clean_rows - decoder_bias).astype(bf16), encoder_weight)
    clean_sent = encode_clean.astype(bf16)
    linear_got = send_mp([jnp.concatenate(pair, axis=1) for pair in zip(blocks_of(linear_sent), blocks_of(clean_sent))])
    clean_got = [piece[:, hidden_width:] for piece in linear_got]
    linear_got = [piece[:, :hidden_width] for piece in linear_got]
    encode_patch = dot((patch.astype(f32) - decoder_bias).astype(bf16), encoder_weight)
    patch_sent = encode_patch.astype(bf16)

    ordered = [jnp.concatenate([block_of(v, m) for m in range(mp_count)], axis=0) for v in (clean, grad)]
    clean_rows, grad_rows = (value.astype(f32) for value in lax.optimization_barrier(ordered))
    weighted_out = output_gain * grad_rows

    mlp_part = dot(hidden_all, down_weight).astype(bf16)
    mlp_out, _ = reduce_latent(mlp_part, None, sides)
    mlp_rows = mlp_out.astype(f32)
    square_out = jnp.sum(mlp_rows * mlp_rows, axis=1, keepdims=True)
    cross_out = jnp.sum(mlp_rows * weighted_out, axis=1, keepdims=True)
    back_part = dot_transposed(mlp_out, down_weight)
    back_sent = jnp.concatenate([back_part.astype(bf16), split_columns([square_out, cross_out])], axis=1)
    back_got = send_mp([back_sent[m * rows : (m + 1) * rows] for m in range(1, mp_count)])
    square_own, cross_own = square_out[:rows], cross_out[:rows]
    for piece in back_got:
        square_piece, cross_piece = join_columns(piece[:, hidden_width:], 2)
        square_own, cross_own = square_own + square_piece, cross_own + cross_piece
    out_scale = lax.rsqrt(square_own / model_width + epsilon)
    hidden_grad = out_scale * total(block_of(linear_part, 0), linear_got) - (
        out_scale * out_scale * out_scale * (cross_own / model_width)
    ) * total(back_part[:rows], [piece[:, :hidden_width] for piece in back_got])
    up_grads = relay_mp((hidden_grad * gelu_value).astype(bf16))
    gate_grad = (hidden_grad * gate_factor).astype(bf16)
    cross_in = jnp.sum(hidden_grad * radial, axis=1, keepdims=True)
    gate_grads = gather_mp(jnp.concatenate([gate_grad, split_columns([cross_in, in_scale, out_scale])], axis=1))
    cross_in, in_scale, out_scale = join_columns(gate_grads[:, hidden_width:], 3)


    patch_got = send_mp(blocks_of(patch_sent))
    latents = encoder_weight.shape[1]
    feature_clean = jnp.maximum(total(block_of(encode_clean, 0), clean_got) + encoder_bias, 0.0)
    feature_patch = jnp.maximum(total(block_of(encode_patch, 0), patch_got) + encoder_bias, 0.0)
    feature_delta = gather_mp((feature_patch - feature_clean).astype(bf16)).astype(f32)

    gate_back = dot_transposed(gate_grads[:, :hidden_width], gate_weight)
    normed_part = dot_transposed(up_grads, up_weight) + gate_back
    normed_grad, cross_in = reduce_latent(normed_part.astype(bf16), cross_in, sides)
    site_grad = (
        grad_rows
        + in_scale * (input_gain * normed_grad.astype(f32))
        - clean_rows * (in_scale * in_scale * (cross_in / model_width))
    ).astype(bf16)
    contribution = feature_delta * dot_transposed(site_grad, decoder_weight)

    effects = jnp.dot(chosen, contribution, precision=lax.Precision.HIGHEST)
    mlp_out, out_scale, effects = lax.optimization_barrier((mlp_out, out_scale, effects))

    def own(value):
        zero = jnp.zeros((), jnp.int32)
        return lax.dynamic_slice(
            value, (own_row, zero), (local_rows, value.shape[1]), allow_negative_indices=False
        )

    block_rows = (
        clean_stream.astype(f32) + own(mlp_out).astype(f32) * own(out_scale) * output_gain
    ).astype(bf16)
    terms = [effects] + [swap(effects, "mp", m) for m in range(1, mp_count)]
    while len(terms) > 1:
        terms = [left + right for left, right in zip(terms[::2], terms[1::2])]
    effects = terms[0]
    return (block_rows, effects[:sequences], effects[sequences:].reshape(sequences, picks, latents))


def solution(mesh):
    in_specs = (
        P("latent", "mp"),
        P("latent", "mp"),
        P("latent", "mp"),
        P("mp"),
        P("mp", "latent"),
        P("mp", "latent"),
        P("latent", "mp"),
        P("mp"),
        P("mp", "latent"),
        P("latent"),
        P("latent", "mp"),
        P("mp"),
        P(),
    )
    out_specs = (P("latent", "mp"), P(None, "latent"), P(None, None, "latent"))
    return jax.shard_map(program, mesh=mesh, in_specs=in_specs, out_specs=out_specs, check_vma=False)
```
